32 devices in a mesh: row: 8 (over y, x, core), col: 4 (over z).
Axes of the slice: x: 2, y: 2, z: 4, core: 2. Of those that a mesh axis runs over, the one named last changes fastest.
Arguments:
- vectors_window: float32 [32, 8, 64, 1024], P(None, 'row', None, 'col'), may hold values from -6 to 6
- column_strip: float32 [32, 8, 64, 1024], P(None, 'row', None, 'col'), may hold values from -6 to 6
- row_strip: float32 [1024, 32, 4, 128], P('row', None, 'col'), may hold values from -6 to 6
- factor: float32 [1024, 1024], P('row', 'col'), may hold values from -2 to 2
- window_start: int32 [1], replicated, may hold values from 1 to 15360
- deflated: int32 [1], replicated, may hold values from 0 to 512
Outputs:
- vectors_updated: float32 [32, 8, 64, 1024], P(None, 'row', None, 'col')
- column_updated: float32 [32, 8, 64, 1024], P(None, 'row', None, 'col')
- row_updated: float32 [1024, 32, 4, 128], P('row', None, 'col')
The draws below stay inside these ranges and needn't reach their ends.
All inputs are finite; a program needn't handle non-finite values.
Results may differ from the reference program's by a relative error of at most 0.0003.
Values sent between devices are 32-bit elements; how exact they have to be, the bound alone decides.
No kernel may reach another device: no remote copies, remote signals or barrier semaphores. Data moves between devices by JAX's collectives and lax.ppermute only.
A program may use at most 64 MiB of HBM per device.

```python
import math
import jax
import jax.numpy as jnp
from jax import lax

W = 1024
BLK = 64
CBLK = 128
ROUNDS = 32
N = 16384
CROUNDS = 32
N_ROW = 8
N_COL = 4


def draw_factor(key, part):
    noise_key, scale_key = jax.random.split(key)
    positions = jnp.arange(W, dtype=jnp.float32) / (W - 1)
    spread = jnp.exp(jax.random.uniform(scale_key, (W,), jnp.float32, -1.15, 1.15))
    entries = jnp.clip(jax.random.normal(noise_key, (W, W), jnp.float32), -5.0, 5.0)
    column_scale = spread * jnp.exp(0.5 * math.log(3.0) * positions) / 1.5
    return (entries * column_scale[None, :] / math.sqrt(W)).astype(jnp.float32)


def block_levels(rng, dims, cuts, smallest, top_value):
    def one(dim, parts):
        steps = jax.random.uniform(jax.random.fold_in(jax.random.fold_in(rng, 6), dim), (parts,), jnp.float32, smallest / len(cuts), top_value / len(cuts))
        return jnp.repeat(jnp.exp(steps), dims[dim] // parts).reshape((-1,) + (1,) * (len(dims) - dim - 1))

    gain = one(*cuts[0])
    for cut in cuts[1:]:
        gain = gain * one(*cut)
    return gain


def normal_values(rng, shape, scale, most, shards=(), kind=jnp.bfloat16):
    gain = block_levels(rng, shape, shards, -0.22, 0.18) if shards else 1.0
    result = jax.random.normal(rng, shape, jnp.float32) * scale * gain
    return jnp.minimum(jnp.maximum(result, -most), most).astype(kind)


def setup_inputs(seed: int = 0) -> dict:
    streams_of = jax.random.split(jax.random.key(seed), 7)
    vectors_window = normal_values(streams_of[0], (ROUNDS, N_ROW, BLK, W), 1.0, 6.0, ((1, 8), (3, 4)), jnp.float32)
    column_strip = normal_values(streams_of[1], (ROUNDS, N_ROW, BLK, W), 1.0, 6.0, ((1, 8), (3, 4)), jnp.float32)
    row_strip = normal_values(streams_of[2], (W, CROUNDS, N_COL, CBLK), 1.0, 6.0, ((0, 8), (2, 4)), jnp.float32)
    factor = draw_factor(jax.random.fold_in(streams_of[6], 71), 0)
    window_start = jax.random.randint(streams_of[4], (1,), 1, N - W + 1).astype(jnp.int32)
    deflated = jax.random.randint(streams_of[5], (1,), 0, W // 2 + 1).astype(jnp.int32)
    return dict(vectors_window=vectors_window, column_strip=column_strip, row_strip=row_strip, factor=factor, window_start=window_start, deflated=deflated)


def reflect(factor, deflated):
    columns = jnp.arange(W, dtype=jnp.int32)
    kept_count = W - deflated[0]
    spike_row = jnp.where(columns < kept_count, factor[0], 0.0)
    squares = jnp.sum(spike_row * spike_row)
    corner = factor[0, 0]
    magnitude = jnp.sqrt(squares + 1e-06)
    signum = jnp.where(corner >= 0, 1.0, -1.0)
    vector = spike_row + jnp.where(columns == 0, signum * magnitude, 0.0)
    denominator = squares + 2.0 * jnp.abs(corner) * magnitude + magnitude * magnitude
    scaling = 2.0 / denominator
    reflected_image = jnp.dot(factor, vector, precision=lax.Precision.HIGHEST)
    return factor - scaling * reflected_image[:, None] * vector[None, :]

def reference(vectors_window, column_strip, row_strip, factor, window_start, deflated):
    highest = lax.Precision.HIGHEST
    rotation = reflect(factor, deflated)
    start_row = window_start[0]
    z_matrix = vectors_window.reshape(N, W)
    vectors_updated = jnp.dot(z_matrix, rotation, precision=highest).reshape(vectors_window.shape)
    strip_matrix = column_strip.reshape(N, W)
    turned = jnp.dot(strip_matrix, rotation, precision=highest)
    row_number = jnp.arange(N, dtype=jnp.int32)
    column_updated = jnp.where(row_number[:, None] < start_row, turned, strip_matrix).reshape(column_strip.shape)
    row_panel = row_strip.reshape(W, N)
    rotated_rows = lax.dot_general(rotation, row_panel, (((0,), (0,)), ((), ())), precision=highest)
    column_number = jnp.arange(N, dtype=jnp.int32)
    row_updated = jnp.where(column_number[None, :] >= start_row + W, rotated_rows, row_panel).reshape(row_strip.shape)
    return (vectors_updated, column_updated, row_updated)
```

```python
import functools

import jax
import jax.numpy as jnp
from jax import lax
from jax.experimental import pallas as pl
from jax.experimental.pallas import tpu as pltpu
from jax.sharding import PartitionSpec as P


LEVELS = 60
TILE = 256
VMEM_LIMIT = 48 * 1024 * 1024
VMEM = pl.BlockSpec(memory_space=pltpu.VMEM)
SMEM = pl.BlockSpec(memory_space=pltpu.SMEM)
ANY = pl.BlockSpec(memory_space=pl.ANY)
F32 = jnp.float32
BF16 = jnp.bfloat16


def exchange(value, axis, bits, size):
    return lax.ppermute(value, axis, [(i, i ^ bits) for i in range(size)])


def split(value):
    high = value.astype(BF16)
    return high, (value - high.astype(F32)).astype(BF16)


def dot(a, b):
    return jnp.dot(a, b, preferred_element_type=F32)


def gather_factor(factor, n_row, n_col):
    blocks = [factor] + [None] * (n_col - 1)
    for bits in range(n_col - 1, 0, -1):
        if bits == (n_col - 1) ^ 1 and n_col > 2:
            continue
        blocks[bits] = exchange(factor, "col", bits, n_col)
    if n_col > 2:
        blocks[(n_col - 1) ^ 1] = exchange(blocks[n_col - 1], "col", 1, n_col)
    own = jnp.stack(blocks)
    pieces = [(own, 0, 0)]
    bits = 1
    while bits < n_row:
        bits *= 2
    if bits == 8 and n_col % 2 == 0:
        half = n_col // 2
        x_side = exchange(own, "row", 2, n_row)
        y_side = exchange(own, "row", 4, n_row)
        first = exchange(y_side[:half], "row", 2, n_row)
        second = exchange(x_side[half:], "row", 4, n_row)
        pieces += [(x_side, 2, 0), (y_side, 4, 0), (first, 6, 0), (second, 6, half)]
    else:
        step = 2
        while step < n_row:
            pieces += [(exchange(a, "row", step, n_row), r ^ step, k) for a, r, k in pieces]
            step *= 2
    if n_row > 1:
        pieces += [(exchange(a, "row", 1, n_row), r ^ 1, k) for a, r, k in pieces]
    return pieces


def reflect_kernel(places, block_rows, scalars, *refs):
    count = len(places)
    sources = refs[:count]
    high_ref, low_ref = refs[count : count + 2]
    (vector_ref,) = refs[count + 2 :]
    row_position, col_position, kept_count = scalars[0], scalars[1], scalars[2]
    n_col, _, local_width = high_ref.shape
    groups = {}
    for source, (row_bits, col_bits) in zip(sources, places):
        groups.setdefault(row_bits, []).append((source, col_bits))
    for row_bits, members in groups.items():

        @pl.when(row_position == row_bits)
        def _():
            for source, col_bits in members:
                for k in range(source.shape[0]):
                    vector_ref[col_position ^ (col_bits + k)] = source[k, 0:1, :]

    corner = vector_ref[0, 0:1, 0:1]
    lane = lax.broadcasted_iota(jnp.int32, (1, local_width), 1)
    squares = jnp.zeros((1, 1), F32)
    for j in range(n_col):
        spike = jnp.where(lane + j * local_width < kept_count, vector_ref[j], 0.0)
        vector_ref[j] = spike
        squares = squares + jnp.sum(spike * spike, axis=1, keepdims=True)
    magnitude = jnp.sqrt(squares + 1e-06)
    signum = jnp.where(corner >= 0, 1.0, -1.0)
    vector_ref[0] = vector_ref[0] + jnp.where(lane == 0, signum * magnitude, 0.0)
    denominator = squares + 2.0 * jnp.abs(corner) * magnitude + magnitude * magnitude
    scaling = 2.0 / denominator
    for row_bits, members in groups.items():
        rows = pl.ds(pl.multiple_of((row_position ^ row_bits) * block_rows, block_rows), block_rows)
        image = jnp.zeros((block_rows, local_width), F32)
        for source, col_bits in members:

            def image_step(k, total):
                return total + source[k] * vector_ref[col_position ^ (col_bits + k)]

            image = lax.fori_loop(0, source.shape[0], image_step, image)
        image = jnp.sum(image, axis=1, keepdims=True) * scaling
        for source, col_bits in members:

            def write_step(k, carry):
                column = col_position ^ (col_bits + k)
                high, low = split(source[k] - image * vector_ref[column])
                high_ref[column, rows, :] = high
                low_ref[column, rows, :] = low
                return carry

            lax.fori_loop(0, source.shape[0], write_step, 0)


def reflect(pieces, scalars, n_row, n_col, block_rows, local_width):
    natural = jax.ShapeDtypeStruct((n_col, n_row * block_rows, local_width), BF16)
    return pl.pallas_call(
        functools.partial(reflect_kernel, [(r, k) for _, r, k in pieces], block_rows),
        in_specs=[SMEM] + [VMEM] * len(pieces),
        out_specs=[VMEM] * 2,
        out_shape=[natural, natural],
        scratch_shapes=[pltpu.VMEM((n_col, 1, local_width), F32)],
        compiler_params=pltpu.CompilerParams(vmem_limit_bytes=VMEM_LIMIT),
        name="reflect",
    )(scalars, *[a for a, _, _ in pieces])


def turn_kernel(masked, n_col, scalars, *refs):
    sources = refs[:n_col]
    high_ref, low_ref = refs[n_col : n_col + 2]
    outs = refs[n_col + 2 : 2 * n_col + 2]
    stacked, result = refs[2 * n_col + 2 :]
    position, threshold = scalars[0], scalars[1]
    rows, local_width = sources[0].shape
    for k in range(n_col):
        high, low = split(sources[k][...])
        stacked[position ^ k, :rows, :] = high
        stacked[position ^ k, rows:, :] = low

    def column_step(j, carry):
        column = position ^ j
        total = jnp.zeros((rows, local_width), F32)
        for k in range(n_col):
            band = pl.ds(k * local_width, local_width)
            both = dot(stacked[k], high_ref[column, band, :])
            total = total + both[rows:] + dot(stacked[k, :rows, :], low_ref[column, band, :]) + both[:rows]
        result[j] = total
        return carry

    lax.fori_loop(0, n_col, column_step, 0)
    for k in range(n_col):
        turned = result[k]
        if masked:
            number = lax.broadcasted_iota(jnp.int32, (rows, local_width), 0)
            turned = jnp.where(number < threshold, turned, sources[k][...])
        outs[k][...] = turned


def turn(sources, high, low, scalars, masked):
    n_col = len(sources)
    rows, local_width = sources[0].shape
    return pl.pallas_call(
        functools.partial(turn_kernel, masked, n_col),
        in_specs=[SMEM] + [VMEM] * (n_col + 2),
        out_specs=[VMEM] * n_col,
        out_shape=[jax.ShapeDtypeStruct((rows, local_width), F32)] * n_col,
        scratch_shapes=[
            pltpu.VMEM((n_col, 2 * rows, local_width), BF16),
            pltpu.VMEM((n_col, rows, local_width), F32),
        ],
        compiler_params=pltpu.CompilerParams(vmem_limit_bytes=VMEM_LIMIT),
        name="turn",
    )(scalars, *sources, high, low)


def stand_kernel(n_row, count, scalars, *refs):
    sources = refs[:n_row]
    high_ref, low_ref = refs[n_row : n_row + 2]
    outs = refs[n_row + 2 : 2 * n_row + 2]
    panel_high, panel_low, result = refs[2 * n_row + 2 :]
    position, threshold = scalars[0], scalars[1]
    n_col, width, local_width = high_ref.shape
    lanes = sources[0].shape[1]
    block_rows = sources[0].shape[0] // count
    for i in range(n_row):
        rows = pl.ds(pl.multiple_of((position ^ i) * block_rows, block_rows), block_rows)
        for t in range(count):
            high, low = split(sources[i][pl.ds(t, block_rows, stride=count), :])
            panel_high[rows, t * lanes : (t + 1) * lanes] = high
            panel_low[rows, t * lanes : (t + 1) * lanes] = low

    def rows_step(j, carry):
        total = jnp.zeros((local_width, count * lanes), F32)
        for k in range(width // TILE):
            band = pl.ds(k * TILE, TILE)
            left = high_ref[j, band, :].T
            total = total + dot(left, panel_low[band, :]) + dot(low_ref[j, band, :].T, panel_high[band, :])
            total = total + dot(left, panel_high[band, :])
        result[pl.ds(pl.multiple_of(j * local_width, local_width), local_width), :] = total
        return carry

    lax.fori_loop(0, n_col, rows_step, 0)
    lane = lax.broadcasted_iota(jnp.int32, (block_rows, lanes), 1)
    for i in range(n_row):
        rows = pl.ds(pl.multiple_of((position ^ i) * block_rows, block_rows), block_rows)
        for t in range(count):
            strided = pl.ds(t, block_rows, stride=count)
            outs[i][strided, :] = jnp.where(
                lane + t * lanes >= threshold,
                result[rows, t * lanes : (t + 1) * lanes],
                sources[i][strided, :],
            )


def stand(sources, high, low, scalars, count):
    n_row = len(sources)
    shape = sources[0].shape
    width = high.shape[1]
    return pl.pallas_call(
        functools.partial(stand_kernel, n_row, count),
        in_specs=[SMEM] + [VMEM] * (n_row + 2),
        out_specs=[VMEM] * n_row,
        out_shape=[jax.ShapeDtypeStruct(shape, F32)] * n_row,
        scratch_shapes=[
            pltpu.VMEM((width, count * shape[1]), BF16),
            pltpu.VMEM((width, count * shape[1]), BF16),
            pltpu.VMEM((width, count * shape[1]), F32),
        ],
        compiler_params=pltpu.CompilerParams(vmem_limit_bytes=VMEM_LIMIT),
        name="stand",
    )(scalars, *sources, high, low)


def place_kernel(groups, axis, tail, scalars, *refs):
    count = sum(len(g) for g in groups)
    pieces = refs[:count]
    position = scalars[0]
    if tail is None:
        target, sems = refs[count:]
    else:
        source, target, sems, kept, tail_sem = refs[count:]
        keep = pl.ds(tail, target.shape[0] - tail)
        fetch = pltpu.make_async_copy(source.at[keep], kept, tail_sem)
        fetch.start()
    copies = []
    for piece, (base, bits) in zip(pieces, [p for g in groups for p in g]):
        size = piece.shape[axis]
        start = base + (position ^ bits) * size
        if axis == 0 and size % 8 == 0 and base % 8 == 0:
            start = pl.multiple_of(start, 8)
        spot = (slice(None),) * axis + (pl.ds(start, size),)
        copies.append(pltpu.make_async_copy(piece, target.at[spot], sems.at[len(copies)]))
    for copy in copies:
        copy.start()
    if tail is not None:
        fetch.wait()
        copies.append(pltpu.make_async_copy(kept, target.at[keep], sems.at[len(copies)]))
        copies[-1].start()
    for copy in copies:
        copy.wait()


def place(groups, pieces, position, shape, axis=0, source=None, tail=None):
    operands = list(pieces)
    in_specs = [SMEM] + [VMEM] * len(pieces)
    scratch = [pltpu.SemaphoreType.DMA((len(pieces) + 1,))]
    if tail is not None:
        operands.append(source)
        in_specs.append(ANY)
        scratch += [pltpu.VMEM((shape[0] - tail,) + shape[1:], F32), pltpu.SemaphoreType.DMA]
    return pl.pallas_call(
        functools.partial(place_kernel, groups, axis, tail),
        in_specs=in_specs,
        out_specs=ANY,
        out_shape=jax.ShapeDtypeStruct(shape, F32),
        scratch_shapes=scratch,
        compiler_params=pltpu.CompilerParams(vmem_limit_bytes=VMEM_LIMIT),
        name="place",
    )(position, *operands)


def below(bound, period, block, position):
    full = bound // period
    return full * block + jnp.clip(bound - full * period - position * block, 0, block)


def body(n_row, n_col, vectors_window, column_strip, row_strip, factor, window_start, deflated):
    row_position = lax.axis_index("row").astype(jnp.int32)
    col_position = lax.axis_index("col").astype(jnp.int32)
    start_row = window_start[0]
    rounds, _, blocks, local_width = vectors_window.shape
    block_rows = factor.shape[0]
    width = block_rows * n_row
    strip_rows, col_rounds, _, col_block = row_strip.shape
    height = rounds * blocks
    vectors = vectors_window.reshape(height, local_width)
    strip = column_strip.reshape(height, local_width)

    pieces = gather_factor(factor, n_row, n_col)

    def rows_in(matrix, base, size):
        parts = [lax.dynamic_slice_in_dim(matrix, base + (col_position ^ k) * size, size) for k in range(n_col)]
        order = range(n_col - 1, 0, -1)
        got = {k: exchange(parts[k], "col", k, n_col) for k in order}
        return [parts[0]] + [got[k] for k in range(1, n_col)]

    def rows_out(parts):
        got = {k: exchange(parts[k], "col", k, n_col) for k in range(n_col - 1, 0, -1)}
        return [parts[0]] + [got[k] for k in range(1, n_col)]

    half = height // 2
    share = half // n_col
    first_in = rows_in(vectors, 0, share)
    second_in = rows_in(vectors, half, share)
    per_device = col_rounds // n_row
    piece_shape = (strip_rows, per_device, 1, col_block)
    flat_shape = (strip_rows * per_device, col_block)
    row_parts = [
        lax.dynamic_slice_in_dim(row_strip, (row_position ^ i) * per_device, per_device, axis=1).reshape(flat_shape)
        for i in range(n_row)
    ]
    row_in = [row_parts[0]] + [exchange(row_parts[i], "row", i, n_row) for i in range(1, n_row)]

    scalars = jnp.stack([row_position, col_position, width - deflated[0]])
    high, low = reflect(pieces, scalars, n_row, n_col, block_rows, local_width)

    col_scalars = jnp.stack([col_position, jnp.int32(0)])
    first_turned = turn(first_in, high, low, col_scalars, False)
    first_out = rows_out(first_turned)
    second_turned = turn(second_in, high, low, col_scalars, False)

    columns_kept = below(start_row + width, n_col * col_block, col_block, col_position)
    row_scalars = jnp.stack([row_position, columns_kept - row_position * (per_device * col_block)])
    stood = stand(row_in, high, low, row_scalars, per_device)
    row_out = [stood[0]] + [exchange(stood[i], "row", i, n_row) for i in range(1, n_row)]

    round_rows = n_row * blocks
    active_rounds = -(-(rounds * round_rows - width) // round_rows)
    levels = min(LEVELS // n_col, active_rounds)
    rows_turned = below(start_row, round_rows, blocks, row_position)
    sizes = [-(-active_rounds * (level + 1) // levels) for level in range(levels)]

    def branch(index, strip, high, low, rows_turned, *second):
        used = sizes[index]
        size = used * blocks // n_col
        strip_in = rows_in(strip, 0, size)
        second_out = rows_out(list(second))
        strip_scalars = jnp.stack([col_position, rows_turned - col_position * size])
        turned = turn(strip_in, high, low, strip_scalars, True)
        strip_out = rows_out(turned)
        groups = [[(0, k) for k in range(n_col)]]
        tail = used * blocks if used < rounds else None
        updated = place(groups, strip_out, col_scalars, strip.shape, source=strip, tail=tail)
        return [updated] + second_out

    used_rounds = -(-start_row // round_rows)
    level = sum((used_rounds > size).astype(jnp.int32) for size in sizes[:-1]) if levels > 1 else jnp.int32(0)
    strip_updated, *second_out = lax.switch(
        level, [functools.partial(branch, i) for i in range(levels)], strip, high, low, rows_turned, *second_turned
    )
    groups = [[(0, k) for k in range(n_col)], [(half, k) for k in range(n_col)]]
    vectors_updated = place(groups, first_out + second_out, col_scalars, vectors.shape)
    row_pieces = [part.reshape(piece_shape) for part in row_out]
    row_updated = place([[(0, i) for i in range(n_row)]], row_pieces, row_scalars, row_strip.shape, axis=1)
    return (
        vectors_updated.reshape(vectors_window.shape),
        strip_updated.reshape(column_strip.shape),
        row_updated,
    )


def solution(mesh):
    n_row, n_col = mesh.shape["row"], mesh.shape["col"]
    return jax.shard_map(
        functools.partial(body, n_row, n_col),
        mesh=mesh,
        in_specs=(
            P(None, "row", None, "col"),
            P(None, "row", None, "col"),
            P("row", None, "col", None),
            P("row", "col"),
            P(),
            P(),
        ),
        out_specs=(
            P(None, "row", None, "col"),
            P(None, "row", None, "col"),
            P("row", None, "col", None),
        ),
        check_vma=False,
    )
```

```python
import functools

import jax
import jax.numpy as jnp
from jax import lax
from jax.experimental import pallas as pl
from jax.experimental.pallas import tpu as pltpu
from jax.sharding import PartitionSpec as P


LEVELS = 60
FRONT = 3
PARTS = 4
TILE = 256
VMEM_LIMIT = 20 * 1024 * 1024
VMEM = pl.BlockSpec(memory_space=pltpu.VMEM)
SMEM = pl.BlockSpec(memory_space=pltpu.SMEM)
ANY = pl.BlockSpec(memory_space=pl.ANY)
F32 = jnp.float32
BF16 = jnp.bfloat16


def exchange(value, axis, bits, size):
    return lax.ppermute(value, axis, [(i, i ^ bits) for i in range(size)])


def split(value):
    high = value.astype(BF16)
    return high, (value - high.astype(F32)).astype(BF16)


def dot(a, b):
    return jnp.dot(a, b, preferred_element_type=F32)


def below(bound, period, block, position):
    full = lax.div(bound, jnp.int32(period))
    return full * block + jnp.clip(bound - full * period - position * block, 0, block)


def gather_factor(factor, n_row, n_col):
    blocks = [factor] + [None] * (n_col - 1)
    for bits in range(n_col - 1, 0, -1):
        if bits == (n_col - 1) ^ 1 and n_col > 2:
            continue
        blocks[bits] = exchange(factor, "col", bits, n_col)
    if n_col > 2:
        blocks[(n_col - 1) ^ 1] = exchange(blocks[n_col - 1], "col", 1, n_col)
    own = jnp.stack(blocks)
    pieces = [(own, 0, 0)]
    bits = 1
    while bits < n_row:
        bits *= 2
    if bits == 8 and n_col % 2 == 0:
        half = n_col // 2
        x_side = exchange(own, "row", 2, n_row)
        y_side = exchange(own, "row", 4, n_row)
        first = exchange(y_side[:half], "row", 2, n_row)
        second = exchange(x_side[half:], "row", 4, n_row)
        pieces += [(x_side, 2, 0), (y_side, 4, 0), (first, 6, 0), (second, 6, half)]
    else:
        step = 2
        while step < n_row:
            pieces += [(exchange(a, "row", step, n_row), r ^ step, k) for a, r, k in pieces]
            step *= 2
    if n_row > 1:
        pieces += [(exchange(a, "row", 1, n_row), r ^ 1, k) for a, r, k in pieces]
    return pieces


def reflect_kernel(places, block_rows, place_ref, deflated_ref, *refs):
    count = len(places)
    sources = refs[:count]
    high_ref, low_ref = refs[count : count + 2]
    (vector_ref,) = refs[count + 2 :]
    row_position, col_position = place_ref[0], place_ref[1]
    n_col, width, local_width = high_ref.shape
    kept_count = width - deflated_ref[0]
    groups = {}
    for source, (row_bits, col_bits) in zip(sources, places):
        groups.setdefault(row_bits, []).append((source, col_bits))
    for row_bits, members in groups.items():

        @pl.when(row_position == row_bits)
        def _():
            for source, col_bits in members:
                for k in range(source.shape[0]):
                    vector_ref[col_position ^ (col_bits + k)] = source[k, 0:1, :]

    corner = vector_ref[0, 0:1, 0:1]
    lane = lax.broadcasted_iota(jnp.int32, (1, local_width), 1)
    squares = jnp.zeros((1, 1), F32)
    for j in range(n_col):
        spike = jnp.where(lane + j * local_width < kept_count, vector_ref[j], 0.0)
        vector_ref[j] = spike
        squares = squares + jnp.sum(spike * spike, axis=1, keepdims=True)
    magnitude = jnp.sqrt(squares + 1e-06)
    signum = jnp.where(corner >= 0, 1.0, -1.0)
    vector_ref[0] = vector_ref[0] + jnp.where(lane == 0, signum * magnitude, 0.0)
    denominator = squares + 2.0 * jnp.abs(corner) * magnitude + magnitude * magnitude
    scaling = 2.0 / denominator
    for row_bits, members in groups.items():
        rows = pl.ds(pl.multiple_of((row_position ^ row_bits) * block_rows, block_rows), block_rows)
        image = jnp.zeros((block_rows, local_width), F32)
        for source, col_bits in members:

            def image_step(k, total):
                return total + source[k] * vector_ref[col_position ^ (col_bits + k)]

            image = lax.fori_loop(0, source.shape[0], image_step, image)
        image = jnp.sum(image, axis=1, keepdims=True) * scaling
        for source, col_bits in members:

            def write_step(k, carry):
                column = col_position ^ (col_bits + k)
                high, low = split(source[k] - image * vector_ref[column])
                high_ref[column, rows, :] = high
                low_ref[column, rows, :] = low
                return carry

            lax.fori_loop(0, source.shape[0], write_step, 0)


def reflect(pieces, position, deflated, n_row, n_col, block_rows, local_width):
    natural = jax.ShapeDtypeStruct((n_col, n_row * block_rows, local_width), BF16)
    return pl.pallas_call(
        functools.partial(reflect_kernel, [(r, k) for _, r, k in pieces], block_rows),
        in_specs=[SMEM] * 2 + [VMEM] * len(pieces),
        out_specs=[VMEM] * 2,
        out_shape=[natural, natural],
        scratch_shapes=[pltpu.VMEM((n_col, 1, local_width), F32)],
        compiler_params=pltpu.CompilerParams(vmem_limit_bytes=VMEM_LIMIT),
        name="reflect",
    )(position, deflated, *[a for a, _, _ in pieces])


def turn_kernel(n_col, bound, place_ref, *refs):
    if bound is not None:
        start_ref, *refs = refs
    sources = refs[:n_col]
    high_ref, low_ref = refs[n_col : n_col + 2]
    outs = refs[n_col + 2 : 2 * n_col + 2]
    stacked, result = refs[2 * n_col + 2 :]
    position = place_ref[1]
    rows, local_width = sources[0].shape
    for k in range(n_col):
        high, low = split(sources[k][...])
        stacked[position ^ k, :rows, :] = high
        stacked[position ^ k, rows:, :] = low

    def column_step(j, carry):
        column = position ^ j
        total = jnp.zeros((rows, local_width), F32)
        for k in range(n_col):
            band = pl.ds(k * local_width, local_width)
            both = dot(stacked[k], high_ref[column, band, :])
            total = total + both[rows:] + dot(stacked[k, :rows, :], low_ref[column, band, :]) + both[:rows]
        result[j] = total
        return carry

    lax.fori_loop(0, n_col, column_step, 0)
    if bound is not None:
        threshold = below(start_ref[0], *bound, place_ref[0]) - position * rows
    for k in range(n_col):
        turned = result[k]
        if bound is not None:
            number = lax.broadcasted_iota(jnp.int32, (rows, local_width), 0)
            turned = jnp.where(number < threshold, turned, sources[k][...])
        outs[k][...] = turned


def turn(sources, high, low, position, start=None, bound=None):
    n_col = len(sources)
    rows, local_width = sources[0].shape
    small = [position] if bound is None else [position, start]
    return pl.pallas_call(
        functools.partial(turn_kernel, n_col, bound),
        in_specs=[SMEM] * len(small) + [VMEM] * (n_col + 2),
        out_specs=[VMEM] * n_col,
        out_shape=[jax.ShapeDtypeStruct((rows, local_width), F32)] * n_col,
        scratch_shapes=[
            pltpu.VMEM((n_col, 2 * rows, local_width), BF16),
            pltpu.VMEM((n_col, rows, local_width), F32),
        ],
        compiler_params=pltpu.CompilerParams(vmem_limit_bytes=VMEM_LIMIT),
        name="turn",
    )(*small, *sources, high, low)


def lead_kernel(n_col, place_ref, *refs):
    sources = refs[:n_col]
    high_ref, low_ref, out, stacked = refs[n_col:]
    position = place_ref[1]
    rows, _ = sources[0].shape
    for k in range(n_col):
        high, low = split(sources[k][...])
        stacked[position ^ k, :rows, :] = high
        stacked[position ^ k, rows:, :] = low
    out[...] = column_of(position ^ (n_col - 1), stacked, high_ref, low_ref)


def column_of(column, stacked, high_ref, low_ref):
    n_col, double, local_width = stacked.shape
    rows = double // 2
    total = jnp.zeros((rows, local_width), F32)
    for k in range(n_col):
        band = pl.ds(k * local_width, local_width)
        both = dot(stacked[k], high_ref[column, band, :])
        total = total + both[rows:] + dot(stacked[k, :rows, :], low_ref[column, band, :]) + both[:rows]
    return total


def follow_kernel(n_col, place_ref, stacked, high_ref, low_ref, *refs):
    outs, result = refs[:-1], refs[-1]
    position = place_ref[1]

    def column_step(j, carry):
        result[j] = column_of(position ^ j, stacked, high_ref, low_ref)
        return carry

    lax.fori_loop(0, n_col - 1, column_step, 0)
    for k in range(n_col - 1):
        outs[k][...] = result[k]


def turn_in_two(sources, high, low, position):
    n_col = len(sources)
    rows, local_width = sources[0].shape
    piece = jax.ShapeDtypeStruct((rows, local_width), F32)
    params = pltpu.CompilerParams(vmem_limit_bytes=VMEM_LIMIT)
    last, stacked = pl.pallas_call(
        functools.partial(lead_kernel, n_col),
        in_specs=[SMEM] + [VMEM] * (n_col + 2),
        out_specs=[VMEM] * 2,
        out_shape=[piece, jax.ShapeDtypeStruct((n_col, 2 * rows, local_width), BF16)],
        compiler_params=params,
        name="lead",
    )(position, *sources, high, low)
    others = pl.pallas_call(
        functools.partial(follow_kernel, n_col),
        in_specs=[SMEM] + [VMEM] * 3,
        out_specs=[VMEM] * (n_col - 1),
        out_shape=[piece] * (n_col - 1),
        scratch_shapes=[pltpu.VMEM((n_col - 1, rows, local_width), F32)],
        compiler_params=params,
        name="follow",
    )(position, stacked, high, low)
    return list(others) + [last]


def stand_kernel(n_row, count, bound, place_ref, start_ref, *refs):
    sources = refs[:n_row]
    high_ref, low_ref = refs[n_row : n_row + 2]
    outs = refs[n_row + 2 : 2 * n_row + 2]
    panel_high, panel_low, result = refs[2 * n_row + 2 :]
    position = place_ref[0]
    n_col, width, local_width = high_ref.shape
    lanes = sources[0].shape[1]
    block_rows = sources[0].shape[0] // count
    for i in range(n_row):
        rows = pl.ds(pl.multiple_of((position ^ i) * block_rows, block_rows), block_rows)
        for t in range(count):
            high, low = split(sources[i][pl.ds(t, block_rows, stride=count), :])
            panel_high[rows, t * lanes : (t + 1) * lanes] = high
            panel_low[rows, t * lanes : (t + 1) * lanes] = low

    def rows_step(j, carry):
        total = jnp.zeros((local_width, count * lanes), F32)
        for k in range(width // TILE):
            band = pl.ds(k * TILE, TILE)
            left = high_ref[j, band, :].T
            total = total + dot(left, panel_low[band, :]) + dot(low_ref[j, band, :].T, panel_high[band, :])
            total = total + dot(left, panel_high[band, :])
        result[pl.ds(pl.multiple_of(j * local_width, local_width), local_width), :] = total
        return carry

    lax.fori_loop(0, n_col, rows_step, 0)
    lane = lax.broadcasted_iota(jnp.int32, (block_rows, lanes), 1)
    threshold = below(start_ref[0] + width, *bound, place_ref[1]) - position * (count * lanes)
    for i in range(n_row):
        rows = pl.ds(pl.multiple_of((position ^ i) * block_rows, block_rows), block_rows)
        for t in range(count):
            strided = pl.ds(t, block_rows, stride=count)
            outs[i][strided, :] = jnp.where(
                lane + t * lanes >= threshold,
                result[rows, t * lanes : (t + 1) * lanes],
                sources[i][strided, :],
            )


def stand(sources, high, low, position, start, count, bound):
    n_row = len(sources)
    shape = sources[0].shape
    width = high.shape[1]
    return pl.pallas_call(
        functools.partial(stand_kernel, n_row, count, bound),
        in_specs=[SMEM] * 2 + [VMEM] * (n_row + 2),
        out_specs=[VMEM] * n_row,
        out_shape=[jax.ShapeDtypeStruct(shape, F32)] * n_row,
        scratch_shapes=[
            pltpu.VMEM((width, count * shape[1]), BF16),
            pltpu.VMEM((width, count * shape[1]), BF16),
            pltpu.VMEM((width, count * shape[1]), F32),
        ],
        compiler_params=pltpu.CompilerParams(vmem_limit_bytes=VMEM_LIMIT),
        name="stand",
    )(position, start, *sources, high, low)


def place_kernel(plans, counts, place_ref, *refs):
    targets, sems = refs[-1 - len(plans) : -1], refs[-1]
    copies = []
    first = 0
    for number, ((groups, axis, which), target) in enumerate(zip(plans, targets)):
        position = place_ref[which]
        spots = [spot for group in groups for spot in group]
        for piece, (base, bits) in zip(refs[first : first + counts[number]], spots):
            size = piece.shape[axis]
            start = base + (position ^ bits) * size
            if axis == 0 and size % 8 == 0 and base % 8 == 0:
                start = pl.multiple_of(start, 8)
            spot = (slice(None),) * axis + (pl.ds(start, size),)
            copies.append(pltpu.make_async_copy(piece, target.at[spot], sems.at[len(copies)]))
        first += counts[number]
    for copy in copies:
        copy.start()
    for copy in copies:
        copy.wait()


def place(plans, pieces, position, shapes, begun=None):
    operands = [piece for part in pieces for piece in part]
    counts = [len(part) for part in pieces]
    in_specs = [SMEM] + [VMEM] * len(operands)
    aliases = {}
    for number, array in (begun or {}).items():
        aliases[1 + len(operands)] = number
        operands.append(array)
        in_specs.append(ANY)
    return pl.pallas_call(
        functools.partial(place_kernel, plans, counts),
        in_specs=in_specs,
        out_specs=[ANY] * len(plans),
        out_shape=[jax.ShapeDtypeStruct(shape, F32) for shape in shapes],
        input_output_aliases=aliases,
        scratch_shapes=[pltpu.SemaphoreType.DMA((sum(counts),))],
        compiler_params=pltpu.CompilerParams(vmem_limit_bytes=VMEM_LIMIT),
        name="place",
    )(position, *operands)


def cut_kernel(spots, axis, which, place_ref, source, *refs):
    outs, sems = refs[:-1], refs[-1]
    position = place_ref[which]
    copies = []
    for out, (base, bits) in zip(outs, spots):
        size = out.shape[axis]
        start = base + (position ^ bits) * size
        if axis == 0 and size % 8 == 0 and base % 8 == 0:
            start = pl.multiple_of(start, 8)
        spot = (slice(None),) * axis + (pl.ds(start, size),)
        copies.append(pltpu.make_async_copy(source.at[spot], out, sems.at[len(copies)]))
    for copy in copies:
        copy.start()
    for copy in copies:
        copy.wait()


def cut(source, spots, sizes, axis, which, position):
    shapes = [source.shape[:axis] + (size,) + source.shape[axis + 1 :] for size in sizes]
    return pl.pallas_call(
        functools.partial(cut_kernel, spots, axis, which),
        in_specs=[SMEM, ANY],
        out_specs=[VMEM] * len(spots),
        out_shape=[jax.ShapeDtypeStruct(shape, F32) for shape in shapes],
        scratch_shapes=[pltpu.SemaphoreType.DMA((len(spots),))],
        compiler_params=pltpu.CompilerParams(vmem_limit_bytes=VMEM_LIMIT),
        name="cut",
    )(position, source)


def keep_kernel(tail, source, target, kept, sem):
    rows = pl.ds(tail, target.shape[0] - tail)
    for copy in (
        pltpu.make_async_copy(source.at[rows], kept, sem),
        pltpu.make_async_copy(kept, target.at[rows], sem),
    ):
        copy.start()
        copy.wait()


def keep(source, tail):
    shape = source.shape
    return pl.pallas_call(
        functools.partial(keep_kernel, tail),
        in_specs=[ANY],
        out_specs=ANY,
        out_shape=jax.ShapeDtypeStruct(shape, F32),
        scratch_shapes=[pltpu.VMEM((shape[0] - tail,) + shape[1:], F32), pltpu.SemaphoreType.DMA],
        compiler_params=pltpu.CompilerParams(vmem_limit_bytes=VMEM_LIMIT),
        name="keep",
    )(source)


def body(n_row, n_col, vectors_window, column_strip, row_strip, factor, window_start, deflated):
    position = jnp.stack([lax.axis_index("row"), lax.axis_index("col")]).astype(jnp.int32)
    rounds, _, blocks, local_width = vectors_window.shape
    block_rows = factor.shape[0]
    width = block_rows * n_row
    strip_rows, col_rounds, _, col_block = row_strip.shape
    height = rounds * blocks
    vectors = vectors_window.reshape(height, local_width)
    strip = column_strip.reshape(height, local_width)

    pieces = gather_factor(factor, n_row, n_col)

    def rows_in(parts):
        got = {k: exchange(parts[k], "col", k, n_col) for k in range(n_col - 1, 0, -1)}
        return [parts[0]] + [got[k] for k in range(1, n_col)]

    front = height * FRONT // PARTS
    sizes = [front // n_col] * n_col + [(height - front) // n_col] * n_col
    spots = [(0, k) for k in range(n_col)] + [(front, k) for k in range(n_col)]
    cuts = cut(vectors, spots, sizes, 0, 1, position)
    first_in = rows_in(cuts[:n_col])
    second_in = rows_in(cuts[n_col:])
    per_device = col_rounds // n_row
    piece_shape = (strip_rows, per_device, 1, col_block)
    flat_shape = (strip_rows * per_device, col_block)
    cuts = cut(row_strip, [(0, i) for i in range(n_row)], [per_device] * n_row, 1, 0, position)
    row_parts = [part.reshape(flat_shape) for part in cuts]
    row_in = [row_parts[0]] + [exchange(row_parts[i], "row", i, n_row) for i in range(1, n_row)]

    high, low = reflect(pieces, position, deflated, n_row, n_col, block_rows, local_width)

    first_turned = turn_in_two(first_in, high, low, position)
    first_out = rows_in(first_turned)
    second_turned = turn(second_in, high, low, position)
    bound = (n_col * col_block, col_block)
    stood = stand(row_in, high, low, position, window_start, per_device, bound)
    row_out = [stood[0]] + [exchange(stood[i], "row", i, n_row) for i in range(1, n_row)]

    round_rows = n_row * blocks
    active_rounds = -(-(rounds * round_rows - width) // round_rows)
    levels = min(LEVELS // n_col, active_rounds)
    sizes = [-(-active_rounds * (level + 1) // levels) for level in range(levels)]

    def branch(index, strip, high, low, position, start, *second):
        used = sizes[index]
        size = used * blocks // n_col
        cuts = cut(strip, [(0, k) for k in range(n_col)], [size] * n_col, 0, 1, position)
        strip_in = rows_in(cuts)
        second_out = rows_in(list(second))
        turned = turn(strip_in, high, low, position, start, (round_rows, blocks))
        strip_out = rows_in(turned)
        begun = None
        if used < rounds:
            begun = {0: keep(strip, used * blocks)}
        groups = [[(0, k) for k in range(n_col)]]
        (strip_updated,) = place([(groups, 0, 1)], [strip_out], position, [strip.shape], begun)
        return [strip_updated] + second_out

    ends = jnp.asarray([size * round_rows for size in sizes[:-1]] or [rounds * round_rows], jnp.int32)
    level = jnp.sum((window_start > ends).astype(jnp.int32))
    branches = [functools.partial(branch, i) for i in range(levels)]
    strip_updated, *second_out = lax.switch(
        level, branches, strip, high, low, position, window_start, *second_turned
    )
    row_pieces = [part.reshape(piece_shape) for part in row_out]
    vectors_updated, row_updated, strip_updated = place(
        [([[(base, k) for k in range(n_col)] for base in (0, front)], 0, 1), ([[(0, i) for i in range(n_row)]], 1, 0), ([], 0, 0)],
        [first_out + second_out, row_pieces, []],
        position,
        [vectors.shape, row_strip.shape, strip.shape],
        {2: strip_updated},
    )
    return (
        vectors_updated.reshape(vectors_window.shape),
        strip_updated.reshape(column_strip.shape),
        row_updated,
    )


def solution(mesh):
    n_row, n_col = mesh.shape["row"], mesh.shape["col"]
    return jax.shard_map(
        functools.partial(body, n_row, n_col),
        mesh=mesh,
        in_specs=(
            P(None, "row", None, "col"),
            P(None, "row", None, "col"),
            P("row", None, "col", None),
            P("row", "col"),
            P(),
            P(),
        ),
        out_specs=(
            P(None, "row", None, "col"),
            P(None, "row", None, "col"),
            P("row", None, "col", None),
        ),
        check_vma=False,
    )
```
